512 devices in a mesh: dp: 16 (over y, z_hi, core), mp: 32 (over z_lo, x).
Axes of the slice: x: 4, y: 4, z: 16 (z_hi: 2, z_lo: 8; z = z_hi * 8 + z_lo), core: 2. Of those that a mesh axis runs over, the one named last changes fastest.
Arguments:
- grads: bfloat16 [16, 16, 32, 256, 256], P('dp', None, 'mp'), may hold values from -18 to 18
- layer_map: int32 [512], replicated, may hold values from 0 to 31, never falling along the last dimension, each value on 1 to 32 neighbouring positions
Outputs:
- roots: float32 [16, 32, 256, 256], P(None, 'mp', 'dp')
The draws below stay inside these ranges and needn't reach their ends.
Inputs may be any that keep to these rules, and one draw needn't show every extreme that they name: `layer_map`: layer numbers never fall along b; every layer 0 to 31 holds 1 to 32 blocks.
All inputs are finite; a program needn't handle non-finite values.
Results may differ from the reference program's by a relative error of at most 0.0003.
Values sent between devices are 32-bit elements; how exact they have to be, the bound alone decides.
No kernel may reach another device: no remote copies, remote signals or barrier semaphores. Data moves between devices by JAX's collectives and lax.ppermute only.
A program may use at most 64 MiB of HBM per device.

```python
import math
import jax
import jax.numpy as jnp
import numpy as np
from jax import lax

ORDER = 256
COLS = 256
BLOCKS_HELD = 16
ITERS = 8
REPLICAS = 16
HOLDERS = 32
LAYERS = 32
BLOCKS = 512


def draw_grads(key, part):
    shape = (REPLICAS, BLOCKS_HELD, HOLDERS, ORDER, COLS)
    first, second = jax.random.split(jax.random.fold_in(key, 17), 2)
    base = jnp.clip(jax.random.normal(first, shape, jnp.float32), -6.0, 6.0)
    logscale = jax.random.uniform(second, (1, BLOCKS_HELD, HOLDERS, ORDER, 1), jnp.float32, math.log(0.3), math.log(3.0))
    return (base * jnp.exp(logscale)).astype(jnp.bfloat16)


def length_profile(amount, total, reach, slope):
    loads = [(1 << 20) // math.isqrt(standing ** slope) + 1 for standing in range(2, amount + 1)]
    surplus, given = total - reach - (amount - 1), [1] * (amount - 1)
    while surplus > 0:
        free = [i for i in range(amount - 1) if given[i] < reach]
        whole, budget = sum([loads[i] for i in free]), surplus
        for i in free:
            more = min(reach - given[i], max(1, budget * loads[i] // whole), surplus)
            given[i] = given[i] + more
            surplus = surplus - more
    return np.array([reach] + given)


def ragged(stream_key, number_of, total, limit, skew):
    if number_of == 2:
        one = jax.random.randint(stream_key, (), max(1, total - limit), min(limit, total - 1) + 1)
        return jnp.stack([one, total - one])
    lengths = jnp.asarray(length_profile(number_of, total, limit, skew), jnp.int32)
    pairs = (number_of - 1) // 2
    donor, sink = lengths[1:1 + 2 * pairs:2], lengths[2:2 + 2 * pairs:2]
    margin = jnp.minimum(donor - 1, limit - sink)
    passed = jax.random.randint(jax.random.fold_in(stream_key, 1), (pairs,), 0, 1 << 20) % (margin + 1)
    lengths = lengths.at[1:1 + 2 * pairs:2].set(donor - passed).at[2:2 + 2 * pairs:2].set(sink + passed)
    return lengths[jax.random.permutation(jax.random.fold_in(stream_key, 2), number_of)]


def setup_inputs(seed: int = 0) -> dict:
    splits = jax.random.split(jax.random.key(seed), 3)
    return {
        "grads": draw_grads(jax.random.fold_in(splits[2], 71), 0),
        "layer_map": jnp.searchsorted(jnp.cumsum(ragged(splits[1], LAYERS, BLOCKS, LAYERS, 2)), jnp.arange(BLOCKS), side="right").astype(jnp.int32),
    }


def newton_root(stats, ridge, live):
    order = stats.shape[-1]
    identity = jnp.eye(order, dtype=jnp.float32)
    damped = jnp.where(live[:, None, None], stats + ridge[:, None, None] * identity, identity)
    frobenius = jnp.sqrt(lax.optimization_barrier(jnp.sum(damped * damped, axis=(1, 2))))
    scaled = 2.5 / frobenius
    current = (scaled ** 0.25)[:, None, None] * identity
    coupled = scaled[:, None, None] * damped
    for _ in range(ITERS):
        factor = 1.25 * identity - 0.25 * coupled
        current = jnp.einsum('sij,sjk->sik', current, factor, precision=lax.Precision.HIGHEST)
        square = jnp.einsum('sij,sjk->sik', factor, factor, precision=lax.Precision.HIGHEST)
        fourth = jnp.einsum('sij,sjk->sik', square, square, precision=lax.Precision.HIGHEST)
        coupled = jnp.einsum('sij,sjk->sik', fourth, coupled, precision=lax.Precision.HIGHEST)
    return current

def reference(grads, layer_map):
    replicas = grads.shape[0]
    order = grads.shape[3]
    columns = grads.shape[4]
    flat = grads.reshape(replicas, BLOCKS, order, columns)

    def stat_block(pieces):
        wide = pieces.astype(jnp.float32)
        return jnp.einsum('ric,rjc->ij', wide, wide, precision=lax.Precision.HIGHEST) / (replicas * columns)
    stats = lax.map(stat_block, jnp.moveaxis(flat, 1, 0))
    traces = jnp.trace(stats, axis1=1, axis2=2)
    layer_ids = jnp.arange(LAYERS, dtype=jnp.int32)
    onehot = (layer_map[:, None] == layer_ids[None, :]).astype(jnp.float32)
    totals = jnp.dot(traces, onehot, precision=lax.Precision.HIGHEST)
    counts = lax.optimization_barrier(jnp.sum(onehot, axis=0))
    layer_ridge = 0.1 * totals / (counts * order)
    block_ridge = jnp.dot(onehot, layer_ridge, precision=lax.Precision.HIGHEST)
    live = jnp.ones((BLOCKS,), dtype=bool)
    roots = newton_root(stats, block_ridge, live)
    return roots.reshape(BLOCKS_HELD, HOLDERS, order, order)
```

```python
import jax
import jax.numpy as jnp
from jax import lax
from jax.experimental import pallas as pl
from jax.experimental.pallas import tpu as pltpu
from jax.sharding import Mesh
from jax.sharding import PartitionSpec as P


ITERS = 8
FULL_STEPS = 1
ORDER = 256
HALF = 128
ROWS = 264
DP = ("y", "zh", "c")
MP = ("zl", "x")


def _iotas(shape):
    return lax.broadcasted_iota(jnp.int32, shape, 0), lax.broadcasted_iota(jnp.int32, shape, 1)


def _nt(a, b):
    return lax.dot_general(a, b, (((1,), (1,)), ((), ())), preferred_element_type=jnp.float32)


def _stats_kernel(where_ref, layers_ref, grad_ref, send_ref, own_ref):
    core, holder = where_ref[0], where_ref[1]
    holders = 32
    blocks = grad_ref.shape[0]
    half = blocks // 2
    row, col = _iotas((HALF, HALF))
    lane = lax.broadcasted_iota(jnp.int32, (1, HALF), 1)
    sums = jnp.zeros((1, HALF), jnp.float32)
    diagonals = []
    for out_ref, first in ((send_ref, (1 - core) * half), (own_ref, core * half)):
        for k in range(half):
            gradient = grad_ref[first + k]
            top = _nt(gradient[:HALF], gradient)
            low = _nt(gradient[HALF:], gradient[HALF:])
            left = top[:, :HALF]
            out_ref[k, 0:HALF, :] = top[:, HALF:]
            out_ref[k, HALF : 2 * HALF, :] = jnp.where(row > col, left, low)
            on = row == col
            diag_left = jnp.sum(jnp.where(on, left, 0.0), axis=0, keepdims=True)
            diag_low = jnp.sum(jnp.where(on, low, 0.0), axis=0, keepdims=True)
            diagonals.append((out_ref, k, diag_left))
            trace = jnp.sum(diag_left + diag_low, axis=1, keepdims=True)
            layer = layers_ref[(first + k) * holders + holder]
            sums = sums + jnp.where(lane == layer, trace, 0.0)
    tail_row, _ = _iotas((8, HALF))
    for out_ref, k, diag_left in diagonals:
        out_ref[k, 2 * HALF :, :] = jnp.where(tail_row == 0, diag_left, jnp.where(tail_row == 1, sums, 0.0))


def _split(a):
    high = a.astype(jnp.bfloat16)
    return high, (a - high.astype(jnp.float32)).astype(jnp.bfloat16)


def _dot(a, b):
    return jnp.dot(a, b, preferred_element_type=jnp.float32)


def _product(a, b):
    return _dot(a[0], b[0]) + (_dot(a[0], b[1]) + _dot(a[1], b[0]))


def _full(a, b):
    return jnp.dot(a, b, precision=lax.Precision.HIGHEST, preferred_element_type=jnp.float32)


def _unpack(packed):
    row, col = _iotas((HALF, HALF))
    corner = packed[0:HALF]
    both = packed[HALF : 2 * HALF]
    flipped = both.T
    left = jnp.where(row > col, both, jnp.where(row < col, flipped, packed[2 * HALF : 2 * HALF + 1]))
    low = jnp.where(row <= col, both, flipped)
    return jnp.concatenate([jnp.concatenate([left, corner], 1), jnp.concatenate([corner.T, low], 1)], 0)


def _solve_kernel(where_ref, layers_ref, map_ref, own_ref, other_ref, sums_ref, out_ref, first_ref):
    core, line, side, holder = where_ref[0], where_ref[1], where_ref[2], where_ref[3]
    count = own_ref.shape[0]
    row, col = _iotas((ORDER, ORDER))
    on = row == col
    lane = lax.broadcasted_iota(jnp.int32, (1, HALF), 1)
    totals = jnp.sum(sums_ref[...], axis=0, keepdims=True) * (1.0 / 4096.0)
    coupled, factor, current = [], [], []
    for k in range(count):
        stats = _unpack((own_ref[k] + other_ref[k]) * (1.0 / 4096.0))
        layer = layers_ref[((core * 4 + line) * count + k) * 32 + holder]
        members = jnp.sum(jnp.where(map_ref[...] == layer, 1.0, 0.0), axis=(0, 1), keepdims=True)
        total = jnp.sum(jnp.where(lane == layer, totals, 0.0), axis=1, keepdims=True)
        ridge = 0.1 * total / (members * ORDER)
        damped = stats + jnp.where(on, ridge, 0.0)
        squares = jnp.sum(damped * damped, axis=(0, 1), keepdims=True)
        scaled = 2.5 / jnp.sqrt(squares)
        root = jnp.sqrt(jnp.sqrt(scaled))
        coupled.append(scaled * damped)
        factor.append(jnp.where(on, 1.25, 0.0) - 0.25 * coupled[k])
        first_ref[k] = root * factor[k]
        current.append(jnp.concatenate([first_ref[k, pl.ds(q * 64 + side * 32, 32), :] for q in range(4)], 0))
    for step in range(ITERS - 1):
        for k in range(count):
            if step < FULL_STEPS:
                square = _full(factor[k], factor[k])
                fourth = _full(square, square)
                coupled[k] = _full(fourth, coupled[k])
            else:
                parts = _split(factor[k])
                square = _split(_product(parts, parts))
                fourth = _split(_product(square, square))
                coupled[k] = _product(fourth, _split(coupled[k]))
            factor[k] = jnp.where(on, 1.25, 0.0) - 0.25 * coupled[k]
        for k in range(count):
            current[k] = _product(_split(current[k]), _split(factor[k]))
    for k in range(count):
        for c in range(2):
            for q in range(4):
                out_ref[c * 4 + q, k] = current[k][(q * 2 + c) * 16 : (q * 2 + c) * 16 + 16]


def _smem():
    return pl.BlockSpec(memory_space=pltpu.SMEM)


def _vmem():
    return pl.BlockSpec(memory_space=pltpu.VMEM)


def local(grads, layer_map):
    gradient = grads[0, :, 0]
    core, line, side = lax.axis_index("c"), lax.axis_index("y"), lax.axis_index("zh")
    holder = lax.axis_index(MP)
    half = gradient.shape[0] // 2
    pack = jax.ShapeDtypeStruct((half, ROWS, HALF), jnp.float32)
    send, own = pl.pallas_call(
        _stats_kernel,
        out_shape=(pack, pack),
        in_specs=[_smem(), _smem(), _vmem()],
        out_specs=(_vmem(), _vmem()),
        compiler_params=pltpu.CompilerParams(vmem_limit_bytes=16 * 2**20),
        name="stats",
    )(jnp.stack([core, holder]).astype(jnp.int32), layer_map, gradient)
    got = lax.ppermute(send, "c", [(0, 1), (1, 0)])
    chip = own + got
    pieces = lax.all_to_all(chip, "y", 0, 0, tiled=True)
    mine = jnp.sum(pieces.reshape(4, half // 4, ROWS, HALF), axis=0)
    other = lax.ppermute(mine, "zh", [(0, 1), (1, 0)])
    row = jnp.broadcast_to(mine[0, 2 * HALF + 1][None, None], (64, 1, HALF))
    sums = lax.all_to_all(row, ("zh", "zl", "x"), 0, 0, tiled=True)
    rows = pl.pallas_call(
        _solve_kernel,
        out_shape=jax.ShapeDtypeStruct((8, half // 4, 16, ORDER), jnp.float32),
        in_specs=[_smem(), _smem(), _vmem(), _vmem(), _vmem(), _vmem()],
        out_specs=_vmem(),
        scratch_shapes=[pltpu.VMEM((half // 4, ORDER, ORDER), jnp.float32)],
        compiler_params=pltpu.CompilerParams(vmem_limit_bytes=16 * 2**20),
        name="solve",
    )(
        jnp.stack([core, line, side, holder]).astype(jnp.int32),
        layer_map,
        layer_map.reshape(4, HALF),
        mine,
        other,
        sums.reshape(64, HALF),
    )
    back = lax.all_to_all(rows, ("c", "y"), 0, 0, tiled=True)
    return back.reshape(16, 1, 16, ORDER)


def solution(mesh):
    torus = Mesh(mesh.devices.reshape(4, 2, 2, 8, 4), ("y", "zh", "c", "zl", "x"))
    in_specs = (P(DP, None, MP, None, None), P())
    out_specs = P(None, MP, DP, None)
    return jax.shard_map(local, mesh=torus, in_specs=in_specs, out_specs=out_specs, check_vma=False)
```

```python
import jax
import jax.numpy as jnp
from jax import lax
from jax.experimental import pallas as pl
from jax.experimental.pallas import tpu as pltpu
from jax.sharding import Mesh
from jax.sharding import PartitionSpec as P


ITERS = 8
FULL_STEPS = 1
ORDER = 256
HALF = 128
ROWS = 264
DP = ("y", "zh", "c")
MP = ("zl", "x")


def _iotas(shape):
    return lax.broadcasted_iota(jnp.int32, shape, 0), lax.broadcasted_iota(jnp.int32, shape, 1)


def _nt(a, b):
    return lax.dot_general(a, b, (((1,), (1,)), ((), ())), preferred_element_type=jnp.float32)


def _stats_kernel(where_ref, layers_ref, grad_ref, send_ref, own_ref):
    core, holder = where_ref[0], where_ref[1]
    holders = 32
    blocks = grad_ref.shape[0]
    half = blocks // 2
    row, col = _iotas((HALF, HALF))
    lane = lax.broadcasted_iota(jnp.int32, (1, HALF), 1)
    sums = jnp.zeros((1, HALF), jnp.float32)
    diagonals = []
    for out_ref, first in ((send_ref, (1 - core) * half), (own_ref, core * half)):
        for k in range(half):
            gradient = grad_ref[first + k]
            top = _nt(gradient[:HALF], gradient)
            low = _nt(gradient[HALF:], gradient[HALF:])
            left = top[:, :HALF]
            out_ref[k, 0:HALF, :] = top[:, HALF:]
            out_ref[k, HALF : 2 * HALF, :] = jnp.where(row > col, left, low)
            on = row == col
            diag_left = jnp.sum(jnp.where(on, left, 0.0), axis=0, keepdims=True)
            diag_low = jnp.sum(jnp.where(on, low, 0.0), axis=0, keepdims=True)
            diagonals.append((out_ref, k, diag_left))
            trace = jnp.sum(diag_left + diag_low, axis=1, keepdims=True)
            layer = layers_ref[(first + k) * holders + holder]
            sums = sums + jnp.where(lane == layer, trace, 0.0)
    tail_row, _ = _iotas((8, HALF))
    for out_ref, k, diag_left in diagonals:
        out_ref[k, 2 * HALF :, :] = jnp.where(tail_row == 0, diag_left, jnp.where(tail_row == 1, sums, 0.0))


def _split(a):
    high = a.astype(jnp.bfloat16)
    return high, (a - high.astype(jnp.float32)).astype(jnp.bfloat16)


def _dot(a, b):
    return jnp.dot(a, b, preferred_element_type=jnp.float32)


def _product(a, b):
    return _dot(a[0], b[0]) + (_dot(a[0], b[1]) + _dot(a[1], b[0]))


def _full(a, b):
    return jnp.dot(a, b, precision=lax.Precision.HIGHEST, preferred_element_type=jnp.float32)


def _unpack(packed):
    row, col = _iotas((HALF, HALF))
    corner = packed[0:HALF]
    both = packed[HALF : 2 * HALF]
    flipped = both.T
    left = jnp.where(row > col, both, jnp.where(row < col, flipped, packed[2 * HALF : 2 * HALF + 1]))
    low = jnp.where(row <= col, both, flipped)
    return jnp.concatenate([jnp.concatenate([left, corner], 1), jnp.concatenate([corner.T, low], 1)], 0)


def _solve_kernel(where_ref, layers_ref, map_ref, own_ref, other_ref, sums_ref, out_ref, first_ref):
    side, block = where_ref[0], where_ref[1]
    row, col = _iotas((ORDER, ORDER))
    on = row == col
    lane = lax.broadcasted_iota(jnp.int32, (1, HALF), 1)
    stats = _unpack((own_ref[...] + other_ref[...]) * (1.0 / 4096.0))
    layer = layers_ref[block]
    members = jnp.sum(jnp.where(map_ref[...] == layer, 1.0, 0.0), axis=(0, 1), keepdims=True)
    totals = jnp.sum(sums_ref[...], axis=0, keepdims=True) * (1.0 / 4096.0)
    total = jnp.sum(jnp.where(lane == layer, totals, 0.0), axis=1, keepdims=True)
    damped = stats + jnp.where(on, 0.1 * total / (members * ORDER), 0.0)
    scaled = 2.5 / jnp.sqrt(jnp.sum(damped * damped, axis=(0, 1), keepdims=True))
    coupled = scaled * damped
    factor = jnp.where(on, 1.25, 0.0) - 0.25 * coupled
    first_ref[...] = jnp.sqrt(jnp.sqrt(scaled)) * factor
    current = jnp.concatenate([first_ref[pl.ds(q * 64 + side * 32, 32), :] for q in range(4)], 0)
    for step in range(ITERS - 1):
        if step < FULL_STEPS:
            square = _full(factor, factor)
            fourth = _full(square, square)
            coupled = _full(fourth, coupled)
        else:
            parts = _split(factor)
            square = _split(_product(parts, parts))
            fourth = _split(_product(square, square))
            coupled = _product(fourth, _split(coupled))
        factor = jnp.where(on, 1.25, 0.0) - 0.25 * coupled
        current = _product(_split(current), _split(factor))
    for c in range(2):
        for q in range(4):
            out_ref[c * 4 + q] = current[(q * 2 + c) * 16 : (q * 2 + c) * 16 + 16]


def _smem():
    return pl.BlockSpec(memory_space=pltpu.SMEM)


def _vmem():
    return pl.BlockSpec(memory_space=pltpu.VMEM)


def local(grads, layer_map):
    gradient = grads[0, :, 0]
    core, line, side = lax.axis_index("c"), lax.axis_index("y"), lax.axis_index("zh")
    holder = lax.axis_index(MP)
    half = gradient.shape[0] // 2
    pack = jax.ShapeDtypeStruct((half, ROWS, HALF), jnp.float32)
    send, own = pl.pallas_call(
        _stats_kernel,
        out_shape=(pack, pack),
        in_specs=[_smem(), _smem(), _vmem()],
        out_specs=(_vmem(), _vmem()),
        compiler_params=pltpu.CompilerParams(vmem_limit_bytes=16 * 2**20),
        name="stats",
    )(jnp.stack([core, holder]).astype(jnp.int32), layer_map, gradient)
    got = lax.ppermute(send, "c", [(0, 1), (1, 0)])
    chip = [own[4 * k : 4 * k + 4] + got[4 * k : 4 * k + 4] for k in range(half // 4)]
    mine, other = [], []
    for k in range(half // 4):
        pieces = lax.all_to_all(chip[k], "y", 0, 0, tiled=True)
        mine.append(jnp.sum(pieces, axis=0))
        other.append(lax.ppermute(mine[k], "zh", [(0, 1), (1, 0)]))
    row = jnp.broadcast_to(mine[0][2 * HALF + 1][None, None], (64, 1, HALF))
    sums = lax.all_to_all(row, ("zh", "zl", "x"), 0, 0, tiled=True).reshape(64, HALF)
    back = []
    for k in range(half // 4):
        block = ((core * (half // 4) + k) * 4 + line) * 32 + holder
        rows = pl.pallas_call(
            _solve_kernel,
            out_shape=jax.ShapeDtypeStruct((8, 16, ORDER), jnp.float32),
            in_specs=[_smem(), _smem()] + [_vmem()] * 4,
            out_specs=_vmem(),
            scratch_shapes=[pltpu.VMEM((ORDER, ORDER), jnp.float32)],
            compiler_params=pltpu.CompilerParams(vmem_limit_bytes=16 * 2**20),
            name="solve",
        )(jnp.stack([side, block]).astype(jnp.int32), layer_map, layer_map.reshape(4, HALF), mine[k], other[k], sums)
        back.append(lax.all_to_all(rows, ("c", "y"), 0, 0, tiled=True).reshape(2, 4, 16, ORDER))
    return jnp.stack(back, axis=1).reshape(16, 1, 16, ORDER)


def solution(mesh):
    torus = Mesh(mesh.devices.reshape(4, 2, 2, 8, 4), ("y", "zh", "c", "zl", "x"))
    in_specs = (P(DP, None, MP, None, None), P())
    out_specs = P(None, MP, DP, None)
    return jax.shard_map(local, mesh=torus, in_specs=in_specs, out_specs=out_specs, check_vma=False)
```

```python
import jax
import jax.numpy as jnp
from jax import lax
from jax.experimental import pallas as pl
from jax.experimental.pallas import tpu as pltpu
from jax.sharding import Mesh
from jax.sharding import PartitionSpec as P

ITERS = 8
FULL_STEPS = 1
ORDER = 256
HALF = 128
ROWS = 520
TAIL = 512
DP = ("y", "zh", "c")
MP = ("zl", "x")


def _iotas(shape):
    return lax.broadcasted_iota(jnp.int32, shape, 0), lax.broadcasted_iota(jnp.int32, shape, 1)


def _nt(a, b):
    return lax.dot_general(a, b, (((1,), (1,)), ((), ())), preferred_element_type=jnp.float32)


def _stats_kernel(where_ref, layers_hbm, grad_hbm, send_ref, own_ref, grad_ref, layers_ref, sems):
    core, holder, holders = where_ref[0], where_ref[1], 32
    blocks = grad_ref.shape[0]
    half, group = blocks // 2, 2
    layers_copy = pltpu.make_async_copy(layers_hbm, layers_ref, sems.at[blocks // group])
    layers_copy.start()
    copies = []
    for n in range(blocks // group):
        first = jnp.where(n * group < half, (1 - core) * half, (core - 1) * half) + n * group
        copies.append(pltpu.make_async_copy(grad_hbm.at[pl.ds(first, group)], grad_ref.at[pl.ds(n * group, group)], sems.at[n]))
        copies[n].start()
    row, col = _iotas((HALF, HALF))
    on = row == col
    lane = lax.broadcasted_iota(jnp.int32, (1, HALF), 1)
    diagonals, traces = [], []
    for n in range(blocks):
        if n % group == 0:
            copies[n // group].wait()
        out_ref, place = (send_ref, n) if n < half else (own_ref, n - half)
        line, start = place // 2, (place % 2) * 2 * HALF
        gradient = grad_ref[n]
        top = _nt(gradient[:HALF], gradient)
        low = _nt(gradient[HALF:], gradient[HALF:])
        left = top[:, :HALF]
        out_ref[line, start : start + HALF, :] = top[:, HALF:]
        out_ref[line, start + HALF : start + 2 * HALF, :] = jnp.where(row > col, left, low)
        diag_left = jnp.sum(jnp.where(on, left, 0.0), axis=0, keepdims=True)
        diag_low = jnp.sum(jnp.where(on, low, 0.0), axis=0, keepdims=True)
        diagonals.append(diag_left)
        traces.append(jnp.sum(diag_left + diag_low, axis=1, keepdims=True))
    layers_copy.wait()
    sums = jnp.zeros((1, HALF), jnp.float32)
    for n in range(blocks):
        block = n + ((1 - core) * half if n < half else (core - 1) * half)
        sums = sums + jnp.where(lane == layers_ref[block * holders + holder], traces[n], 0.0)
    tail_row, _ = _iotas((8, HALF))
    for n in range(0, blocks, 2):
        out_ref, line = (send_ref, n // 2) if n < half else (own_ref, (n - half) // 2)
        tail = jnp.where(tail_row == 1, diagonals[n + 1], jnp.where(tail_row == 2, sums, 0.0))
        out_ref[line, TAIL:, :] = jnp.where(tail_row == 0, diagonals[n], tail)


def _split(a):
    high = a.astype(jnp.bfloat16)
    return high, (a - high.astype(jnp.float32)).astype(jnp.bfloat16)


def _dot(a, b):
    return jnp.dot(a, b, preferred_element_type=jnp.float32)


def _product(a, b):
    return _dot(a[0], b[0]) + (_dot(a[0], b[1]) + _dot(a[1], b[0]))


def _full(a, b):
    return jnp.dot(a, b, precision=lax.Precision.HIGHEST, preferred_element_type=jnp.float32)


def _unpack(corner, both, diagonal):
    row, col = _iotas((HALF, HALF))
    flipped = both.T
    left = jnp.where(row > col, both, jnp.where(row < col, flipped, diagonal))
    low = jnp.where(row <= col, both, flipped)
    return jnp.concatenate([jnp.concatenate([left, corner], 1), jnp.concatenate([corner.T, low], 1)], 0)


def _factor(on, coupled):
    return jnp.where(on, 1.25, 0.0) - 0.25 * coupled


def _solve_kernel(where_ref, layers_ref, map_ref, own_ref, other_ref, sums_ref, out_ref, first_ref):
    core, line, side, holder = where_ref[0], where_ref[1], where_ref[2], where_ref[3]
    pair = range(2)
    row, col = _iotas((ORDER, ORDER))
    on = row == col
    lane = lax.broadcasted_iota(jnp.int32, (1, HALF), 1)
    totals = jnp.sum(sums_ref[...], axis=0, keepdims=True) * (1.0 / 4096.0)
    coupled, factor, current = [], [], []
    for k in pair:
        corner, both, diagonal = (
            (own_ref[rows, :] + other_ref[rows, :]) * (1.0 / 4096.0)
            for rows in (
                slice(k * 2 * HALF, k * 2 * HALF + HALF),
                slice(k * 2 * HALF + HALF, (k + 1) * 2 * HALF),
                slice(TAIL + k, TAIL + k + 1),
            )
        )
        layer = layers_ref[((core * 4 + line) * 2 + k) * 32 + holder]
        members = jnp.sum(jnp.where(map_ref[...] == layer, 1.0, 0.0), axis=(0, 1), keepdims=True)
        total = jnp.sum(jnp.where(lane == layer, totals, 0.0), axis=1, keepdims=True)
        damped = _unpack(corner, both, diagonal) + jnp.where(on, 0.1 * total / (members * ORDER), 0.0)
        scaled = 2.5 / jnp.sqrt(jnp.sum(damped * damped, axis=(0, 1), keepdims=True))
        coupled.append(scaled * damped)
        factor.append(_factor(on, coupled[k]))
        first_ref[k] = jnp.sqrt(jnp.sqrt(scaled)) * factor[k]
        current.append(jnp.concatenate([first_ref[k, pl.ds(q * 64 + side * 32, 32), :] for q in range(4)], 0))
    for step in range(ITERS - 1):
        if step < FULL_STEPS:
            square = [_full(factor[k], factor[k]) for k in pair]
            fourth = [_full(square[k], square[k]) for k in pair]
            coupled = [_full(fourth[k], coupled[k]) for k in pair]
        else:
            parts = [_split(factor[k]) for k in pair]
            square = [_split(_product(parts[k], parts[k])) for k in pair]
            fourth = [_split(_product(square[k], square[k])) for k in pair]
            coupled = [_product(fourth[k], _split(coupled[k])) for k in pair]
        factor = [_factor(on, coupled[k]) for k in pair]
        current = [_product(_split(current[k]), _split(factor[k])) for k in pair]
    for k in pair:
        for c in range(2):
            for q in range(4):
                out_ref[c * 4 + q, k] = current[k][(q * 2 + c) * 16 : (q * 2 + c) * 16 + 16]


def _smem():
    return pl.BlockSpec(memory_space=pltpu.SMEM)


def _hbm():
    return pl.BlockSpec(memory_space=pltpu.HBM)


def _vmem():
    return pl.BlockSpec(memory_space=pltpu.VMEM)


def local(grads, layer_map):
    gradient = grads[0, :, 0]
    core, line, side = lax.axis_index("c"), lax.axis_index("y"), lax.axis_index("zh")
    holder = lax.axis_index(MP)
    half = gradient.shape[0] // 2
    pack = jax.ShapeDtypeStruct((half // 2, ROWS, HALF), jnp.float32)
    send, own = pl.pallas_call(
        _stats_kernel,
        out_shape=(pack, pack),
        in_specs=[_smem(), _hbm(), _hbm()],
        out_specs=(_vmem(), _vmem()),
        scratch_shapes=[
            pltpu.VMEM(gradient.shape, gradient.dtype),
            pltpu.SMEM(layer_map.shape, layer_map.dtype),
            pltpu.SemaphoreType.DMA((gradient.shape[0] // 2 + 1,)),
        ],
        compiler_params=pltpu.CompilerParams(vmem_limit_bytes=52000 * 2**10),
        name="stats",
    )(jnp.stack([core, holder]).astype(jnp.int32), layer_map, gradient)
    got = lax.ppermute(send, "c", [(0, 1), (1, 0)])
    chip = own + got
    pieces = lax.all_to_all(chip, "y", 0, 0, tiled=True)
    mine = jnp.sum(pieces, axis=0)
    other = lax.ppermute(mine, "zh", [(0, 1), (1, 0)])
    row = jnp.broadcast_to(mine[TAIL + 2][None, None], (64, 1, HALF))
    sums = lax.all_to_all(row, ("zh", "zl", "x"), 0, 0, tiled=True)
    rows = pl.pallas_call(
        _solve_kernel,
        out_shape=jax.ShapeDtypeStruct((8, half // 4, 16, ORDER), jnp.float32),
        in_specs=[_smem(), _smem(), _vmem(), _vmem(), _vmem(), _vmem()],
        out_specs=_vmem(),
        scratch_shapes=[pltpu.VMEM((half // 4, ORDER, ORDER), jnp.float32)],
        compiler_params=pltpu.CompilerParams(vmem_limit_bytes=16 * 2**20),
        name="solve",
    )(
        jnp.stack([core, line, side, holder]).astype(jnp.int32),
        layer_map,
        layer_map.reshape(4, HALF),
        mine,
        other,
        sums.reshape(64, HALF),
    )
    back = lax.all_to_all(rows, ("c", "y"), 0, 0, tiled=True)
    return back.reshape(16, 1, 16, ORDER)


def solution(mesh):
    torus = Mesh(mesh.devices.reshape(4, 2, 2, 8, 4), ("y", "zh", "c", "zl", "x"))
    in_specs = (P(DP, None, MP, None, None), P())
    out_specs = P(None, MP, DP, None)
    return jax.shard_map(local, mesh=torus, in_specs=in_specs, out_specs=out_specs, check_vma=False)
```

```python
import jax
import jax.numpy as jnp
from jax import lax
from jax.experimental import pallas as pl
from jax.experimental.pallas import tpu as pltpu
from jax.sharding import Mesh
from jax.sharding import PartitionSpec as P

ITERS = 8
FULL_STEPS = 1
ORDER = 256
HALF = 128
ROWS = 520
TAIL = 512
DP = ("y", "zh", "c")
MP = ("zl", "x")


def _iotas(shape):
    return lax.broadcasted_iota(jnp.int32, shape, 0), lax.broadcasted_iota(jnp.int32, shape, 1)


def _nt(a, b):
    return lax.dot_general(a, b, (((1,), (1,)), ((), ())), preferred_element_type=jnp.float32)


def _stats_kernel(where_ref, grad_ref, send_ref, own_ref):
    core = where_ref[0]
    blocks = grad_ref.shape[0]
    half = blocks // 2
    row, col = _iotas((HALF, HALF))
    on = row == col
    lane = lax.broadcasted_iota(jnp.int32, (1, HALF), 1)
    diagonals, traces = [], jnp.zeros((1, HALF), jnp.float32)
    for n in range(blocks):
        out_ref, place = (send_ref, n) if n < half else (own_ref, n - half)
        line, start = place // 2, (place % 2) * 2 * HALF
        block = n + ((1 - core) * half if n < half else (core - 1) * half)
        gradient = grad_ref[block]
        top = _nt(gradient[:HALF], gradient)
        low = _nt(gradient[HALF:], gradient[HALF:])
        left = top[:, :HALF]
        out_ref[line, start : start + HALF, :] = top[:, HALF:]
        out_ref[line, start + HALF : start + 2 * HALF, :] = jnp.where(row > col, left, low)
        diag_left = jnp.sum(jnp.where(on, left, 0.0), axis=0, keepdims=True)
        diag_low = jnp.sum(jnp.where(on, low, 0.0), axis=0, keepdims=True)
        diagonals.append(diag_left)
        traces = traces + jnp.where(lane == block, jnp.sum(diag_left + diag_low, axis=1, keepdims=True), 0.0)
    tail_row, _ = _iotas((8, HALF))
    for n in range(0, blocks, 2):
        out_ref, line = (send_ref, n // 2) if n < half else (own_ref, (n - half) // 2)
        tail = jnp.where(tail_row == 1, diagonals[n + 1], jnp.where(tail_row == 2, traces, 0.0))
        out_ref[line, TAIL:, :] = jnp.where(tail_row == 0, diagonals[n], tail)


def _split(a):
    high = a.astype(jnp.bfloat16)
    return high, (a - high.astype(jnp.float32)).astype(jnp.bfloat16)


def _dot(a, b):
    return jnp.dot(a, b, preferred_element_type=jnp.float32)


def _product(a, b):
    return _dot(a[0], b[0]) + (_dot(a[0], b[1]) + _dot(a[1], b[0]))


def _full(a, b):
    return jnp.dot(a, b, precision=lax.Precision.HIGHEST, preferred_element_type=jnp.float32)


def _unpack(corner, both, diagonal):
    row, col = _iotas((HALF, HALF))
    flipped = both.T
    left = jnp.where(row > col, both, jnp.where(row < col, flipped, diagonal))
    low = jnp.where(row <= col, both, flipped)
    return jnp.concatenate([jnp.concatenate([left, corner], 1), jnp.concatenate([corner.T, low], 1)], 0)


def _factor(on, coupled):
    return jnp.where(on, 1.25, 0.0) - 0.25 * coupled


def _solve_kernel(where_ref, map_ref, own_ref, other_ref, traces_ref, out_ref, first_ref):
    side = where_ref[0]
    pair = range(2)
    row, col = _iotas((ORDER, ORDER))
    on = row == col
    coupled, factor, current = [], [], []
    for k in pair:
        corner, both, diagonal = (
            (own_ref[rows, :] + other_ref[rows, :]) * (1.0 / 4096.0)
            for rows in (
                slice(k * 2 * HALF, k * 2 * HALF + HALF),
                slice(k * 2 * HALF + HALF, (k + 1) * 2 * HALF),
                slice(TAIL + k, TAIL + k + 1),
            )
        )
        held = map_ref[...] == where_ref[1 + k]
        members = jnp.sum(jnp.where(held, 0.5, 0.0), axis=(0, 1), keepdims=True)
        total = jnp.sum(jnp.where(held, traces_ref[...], 0.0), axis=(0, 1), keepdims=True) * (1.0 / 4096.0)
        damped = _unpack(corner, both, diagonal) + jnp.where(on, 0.1 * total / (members * ORDER), 0.0)
        scaled = 2.5 / jnp.sqrt(jnp.sum(damped * damped, axis=(0, 1), keepdims=True))
        coupled.append(scaled * damped)
        factor.append(_factor(on, coupled[k]))
        first_ref[k] = jnp.sqrt(jnp.sqrt(scaled)) * factor[k]
        current.append(jnp.concatenate([first_ref[k, pl.ds(q * 64 + side * 32, 32), :] for q in range(4)], 0))
    for step in range(ITERS - 1):
        if step < FULL_STEPS:
            square = [_full(factor[k], factor[k]) for k in pair]
            fourth = [_full(square[k], square[k]) for k in pair]
            coupled = [_full(fourth[k], coupled[k]) for k in pair]
        else:
            parts = [_split(factor[k]) for k in pair]
            square = [_split(_product(parts[k], parts[k])) for k in pair]
            fourth = [_split(_product(square[k], square[k])) for k in pair]
            coupled = [_product(fourth[k], _split(coupled[k])) for k in pair]
        factor = [_factor(on, coupled[k]) for k in pair]
        current = [_product(_split(current[k]), _split(factor[k])) for k in pair]
    for k in pair:
        for c in range(2):
            for q in range(4):
                out_ref[c * 4 + q, k] = current[k][(q * 2 + c) * 16 : (q * 2 + c) * 16 + 16]


def _smem():
    return pl.BlockSpec(memory_space=pltpu.SMEM)


def _vmem():
    return pl.BlockSpec(memory_space=pltpu.VMEM)


def local(grads, layer_map):
    gradient = grads[0, :, 0]
    core, line, side = lax.axis_index("c"), lax.axis_index("y"), lax.axis_index("zh")
    holder = lax.axis_index(MP)
    half = gradient.shape[0] // 2
    pack = jax.ShapeDtypeStruct((half // 2, ROWS, HALF), jnp.float32)
    send, own = pl.pallas_call(
        _stats_kernel,
        out_shape=(pack, pack),
        in_specs=[_smem(), _vmem()],
        out_specs=(_vmem(), _vmem()),
        compiler_params=pltpu.CompilerParams(vmem_limit_bytes=16 * 2**20),
        name="stats",
    )(core.astype(jnp.int32).reshape(1), gradient)
    got = lax.ppermute(send, "c", [(0, 1), (1, 0)])
    chip = own + got
    pieces = lax.all_to_all(chip, "y", 0, 0, tiled=True)
    mine = jnp.sum(pieces, axis=0)
    other = lax.ppermute(mine, "zh", [(0, 1), (1, 0)])
    row = jnp.broadcast_to(mine[TAIL + 2][None, None], (64, 1, HALF))
    traces = lax.all_to_all(row, ("zh", "zl", "x"), 0, 0, tiled=True).reshape(64, HALF)
    layers = layer_map.reshape(2 * half, 32)
    layer_of = jnp.pad(jnp.tile(layers.T, (2, 1)), ((0, 0), (0, HALF - 2 * half)), constant_values=-1)
    block = core * half + line * 2
    pair = lax.dynamic_slice(layers, (block, holder), (2, 1)).reshape(2)
    rows = pl.pallas_call(
        _solve_kernel,
        out_shape=jax.ShapeDtypeStruct((8, half // 4, 16, ORDER), jnp.float32),
        in_specs=[_smem()] + [_vmem()] * 4,
        out_specs=_vmem(),
        scratch_shapes=[pltpu.VMEM((half // 4, ORDER, ORDER), jnp.float32)],
        compiler_params=pltpu.CompilerParams(vmem_limit_bytes=16 * 2**20),
        name="solve",
    )(jnp.concatenate([side.astype(jnp.int32).reshape(1), pair]), layer_of, mine, other, traces)
    back = lax.all_to_all(rows, ("c", "y"), 0, 0, tiled=True)
    return back.reshape(16, 1, 16, ORDER)


def solution(mesh):
    torus = Mesh(mesh.devices.reshape(4, 2, 2, 8, 4), ("y", "zh", "c", "zl", "x"))
    in_specs = (P(DP, None, MP, None, None), P())
    out_specs = P(None, MP, DP, None)
    return jax.shard_map(local, mesh=torus, in_specs=in_specs, out_specs=out_specs, check_vma=False)
```

```python
import jax
import jax.numpy as jnp
from jax import lax
from jax.experimental import pallas as pl
from jax.experimental.pallas import tpu as pltpu
from jax.sharding import Mesh
from jax.sharding import PartitionSpec as P

ITERS = 8
ORDER = 256
HALF = 128
ROWS = 520
TAIL = 512
DP = ("y", "zh", "c")
MP = ("zl", "x")


def _iotas(shape):
    return lax.broadcasted_iota(jnp.int32, shape, 0), lax.broadcasted_iota(jnp.int32, shape, 1)


def _nt(a, b):
    return lax.dot_general(a, b, (((1,), (1,)), ((), ())), preferred_element_type=jnp.float32)


def _stats_kernel(where_ref, grad_ref, send_ref, own_ref):
    core = where_ref[0]
    blocks = grad_ref.shape[0]
    half = blocks // 2
    row, col = _iotas((HALF, HALF))
    on = row == col
    lane = lax.broadcasted_iota(jnp.int32, (1, HALF), 1)
    diagonals, traces = [], jnp.zeros((1, HALF), jnp.float32)
    for n in range(blocks):
        out_ref, place = (send_ref, n) if n < half else (own_ref, n - half)
        line, start = place // 2, (place % 2) * 2 * HALF
        block = n + ((1 - core) * half if n < half else (core - 1) * half)
        gradient = grad_ref[block]
        top = _nt(gradient[:HALF], gradient)
        low = _nt(gradient[HALF:], gradient[HALF:])
        left = top[:, :HALF]
        out_ref[line, start : start + HALF, :] = top[:, HALF:]
        out_ref[line, start + HALF : start + 2 * HALF, :] = jnp.where(row > col, left, low)
        diag_left = jnp.sum(jnp.where(on, left, 0.0), axis=0, keepdims=True)
        diag_low = jnp.sum(jnp.where(on, low, 0.0), axis=0, keepdims=True)
        diagonals.append(diag_left)
        traces = traces + jnp.where(lane == block, jnp.sum(diag_left + diag_low, axis=1, keepdims=True), 0.0)
    tail_row, _ = _iotas((8, HALF))
    for n in range(0, blocks, 2):
        out_ref, line = (send_ref, n // 2) if n < half else (own_ref, (n - half) // 2)
        tail = jnp.where(tail_row == 1, diagonals[n + 1], jnp.where(tail_row == 2, traces, 0.0))
        out_ref[line, TAIL:, :] = jnp.where(tail_row == 0, diagonals[n], tail)


def _split(a):
    high = a.astype(jnp.bfloat16)
    return high, (a - high.astype(jnp.float32)).astype(jnp.bfloat16)


def _dot(a, b):
    return jnp.dot(a, b, preferred_element_type=jnp.float32)


def _product(a, b):
    return _dot(a[0], b[0]) + (_dot(a[0], b[1]) + _dot(a[1], b[0]))


def _unpack(corner, both, diagonal):
    row, col = _iotas((HALF, HALF))
    flipped = both.T
    left = jnp.where(row > col, both, jnp.where(row < col, flipped, diagonal))
    low = jnp.where(row <= col, both, flipped)
    return jnp.concatenate([jnp.concatenate([left, corner], 1), jnp.concatenate([corner.T, low], 1)], 0)


def _solve_kernel(where_ref, map_ref, own_ref, other_ref, traces_ref, out_ref, first_ref):
    side = where_ref[0]
    pair = range(2)
    row, col = _iotas((ORDER, ORDER))
    on = row == col
    coupled, current = [], []
    for k in pair:
        corner, both, diagonal = (
            (own_ref[rows, :] + other_ref[rows, :]) * (1.0 / 4096.0)
            for rows in (
                slice(k * 2 * HALF, k * 2 * HALF + HALF),
                slice(k * 2 * HALF + HALF, (k + 1) * 2 * HALF),
                slice(TAIL + k, TAIL + k + 1),
            )
        )
        held = map_ref[...] == where_ref[1 + k]
        members = jnp.sum(jnp.where(held, 0.5, 0.0), axis=(0, 1), keepdims=True)
        total = jnp.sum(jnp.where(held, traces_ref[...], 0.0), axis=(0, 1), keepdims=True) * (1.0 / 4096.0)
        damped = _unpack(corner, both, diagonal) + jnp.where(on, 0.1 * total / (members * ORDER), 0.0)
        scaled = 2.5 / jnp.sqrt(jnp.sum(damped * damped, axis=(0, 1), keepdims=True))
        coupled.append(scaled * damped)
        first_ref[k] = jnp.sqrt(jnp.sqrt(scaled)) * (jnp.where(on, 1.25, 0.0) - 0.25 * coupled[k])
        current.append(jnp.concatenate([first_ref[k, pl.ds(q * 64 + side * 32, 32), :] for q in range(4)], 0))
    parts = [_split(coupled[k]) for k in pair]
    for _ in range(ITERS - 1):
        once = [0.0625 * _product(parts[k], parts[k]) - 0.625 * coupled[k] for k in pair]
        split = [_split(once[k]) for k in pair]
        twice = [_split(3.125 * once[k] + _product(split[k], split[k])) for k in pair]
        coupled = [2.44140625 * coupled[k] + _product(twice[k], parts[k]) for k in pair]
        parts = [_split(coupled[k]) for k in pair]
        current = [1.25 * current[k] - 0.25 * _product(_split(current[k]), parts[k]) for k in pair]
    for k in pair:
        for c in range(2):
            for q in range(4):
                out_ref[c * 4 + q, k] = current[k][(q * 2 + c) * 16 : (q * 2 + c) * 16 + 16]


def _smem():
    return pl.BlockSpec(memory_space=pltpu.SMEM)


def _vmem():
    return pl.BlockSpec(memory_space=pltpu.VMEM)


def local(grads, layer_map):
    gradient = grads[0, :, 0]
    core, line, side = lax.axis_index("c"), lax.axis_index("y"), lax.axis_index("zh")
    holder = lax.axis_index(MP)
    half = gradient.shape[0] // 2
    pack = jax.ShapeDtypeStruct((half // 2, ROWS, HALF), jnp.float32)
    send, own = pl.pallas_call(
        _stats_kernel,
        out_shape=(pack, pack),
        in_specs=[_smem(), _vmem()],
        out_specs=(_vmem(), _vmem()),
        compiler_params=pltpu.CompilerParams(vmem_limit_bytes=16 * 2**20),
        name="stats",
    )(core.astype(jnp.int32).reshape(1), gradient)
    got = lax.ppermute(send, "c", [(0, 1), (1, 0)])
    chip = own + got
    pieces = lax.all_to_all(chip, "y", 0, 0, tiled=True)
    mine = jnp.sum(pieces, axis=0)
    other = lax.ppermute(mine, "zh", [(0, 1), (1, 0)])
    row = jnp.broadcast_to(mine[TAIL + 2][None, None], (64, 1, HALF))
    traces = lax.all_to_all(row, ("zh", "zl", "x"), 0, 0, tiled=True).reshape(64, HALF)
    layers = layer_map.reshape(2 * half, 32)
    layer_of = jnp.pad(jnp.tile(layers.T, (2, 1)), ((0, 0), (0, HALF - 2 * half)), constant_values=-1)
    block = core * half + line * 2
    pair = lax.dynamic_slice(layers, (block, holder), (2, 1)).reshape(2)
    rows = pl.pallas_call(
        _solve_kernel,
        out_shape=jax.ShapeDtypeStruct((8, half // 4, 16, ORDER), jnp.float32),
        in_specs=[_smem()] + [_vmem()] * 4,
        out_specs=_vmem(),
        scratch_shapes=[pltpu.VMEM((half // 4, ORDER, ORDER), jnp.float32)],
        compiler_params=pltpu.CompilerParams(vmem_limit_bytes=16 * 2**20),
        name="solve",
    )(jnp.concatenate([side.astype(jnp.int32).reshape(1), pair]), layer_of, mine, other, traces)
    back = lax.all_to_all(rows, ("c", "y"), 0, 0, tiled=True)
    return back.reshape(16, 1, 16, ORDER)


def solution(mesh):
    torus = Mesh(mesh.devices.reshape(4, 2, 2, 8, 4), ("y", "zh", "c", "zl", "x"))
    in_specs = (P(DP, None, MP, None, None), P())
    out_specs = P(None, MP, DP, None)
    return jax.shard_map(local, mesh=torus, in_specs=in_specs, out_specs=out_specs, check_vma=False)
```

```python
import jax
import jax.numpy as jnp
from jax import lax
from jax.experimental import pallas as pl
from jax.experimental.pallas import tpu as pltpu
from jax.sharding import Mesh
from jax.sharding import PartitionSpec as P


ITERS = 8
ORDER = 256
HALF = 128
ROWS = 520
TAIL = 512
DP = ("y", "zh", "c")
MP = ("zl", "x")


def _iotas(shape):
    return lax.broadcasted_iota(jnp.int32, shape, 0), lax.broadcasted_iota(jnp.int32, shape, 1)


def _nt(a, b):
    return lax.dot_general(a, b, (((1,), (1,)), ((), ())), preferred_element_type=jnp.float32)


def _stats_kernel(where_ref, grad_ref, send_ref, own_ref):
    core = where_ref[0]
    blocks = grad_ref.shape[0]
    half = blocks // 2
    row, col = _iotas((HALF, HALF))
    on = row == col
    lane = lax.broadcasted_iota(jnp.int32, (1, HALF), 1)
    diagonals, traces = [], jnp.zeros((1, HALF), jnp.float32)
    for n in range(blocks):
        out_ref, place = (send_ref, n) if n < half else (own_ref, n - half)
        line, start = place // 2, (place % 2) * 2 * HALF
        block = n + ((1 - core) * half if n < half else (core - 1) * half)
        gradient = grad_ref[block]
        top = _nt(gradient[:HALF], gradient)
        low = _nt(gradient[HALF:], gradient[HALF:])
        left = top[:, :HALF]
        out_ref[line, start : start + HALF, :] = top[:, HALF:]
        out_ref[line, start + HALF : start + 2 * HALF, :] = jnp.where(row > col, left, low)
        diag_left = jnp.sum(jnp.where(on, left, 0.0), axis=0, keepdims=True)
        diag_low = jnp.sum(jnp.where(on, low, 0.0), axis=0, keepdims=True)
        diagonals.append(diag_left)
        traces = traces + jnp.where(lane == block, jnp.sum(diag_left + diag_low, axis=1, keepdims=True), 0.0)
    tail_row, _ = _iotas((8, HALF))
    for n in range(0, blocks, 2):
        out_ref, line = (send_ref, n // 2) if n < half else (own_ref, (n - half) // 2)
        tail = jnp.where(tail_row == 1, diagonals[n + 1], jnp.where(tail_row == 2, traces, 0.0))
        out_ref[line, TAIL:, :] = jnp.where(tail_row == 0, diagonals[n], tail)


def _split(a):
    high = a.astype(jnp.bfloat16)
    return high, (a - high.astype(jnp.float32)).astype(jnp.bfloat16)


def _dot(a, b):
    return jnp.dot(a, b, preferred_element_type=jnp.float32)


def _product(a, b):
    return _dot(a[0], b[0]) + (_dot(a[0], b[1]) + _dot(a[1], b[0]))


def _unpack(corner, both, diagonal):
    row, col = _iotas((HALF, HALF))
    flipped = both.T
    left = jnp.where(row > col, both, jnp.where(row < col, flipped, diagonal))
    low = jnp.where(row <= col, both, flipped)
    return jnp.concatenate([jnp.concatenate([left, corner], 1), jnp.concatenate([corner.T, low], 1)], 0)


def _prepare_kernel(own_ref, other_ref, stats_ref, square_ref, norms_ref):
    row, col = _iotas((ORDER, ORDER))
    norm_row, _ = _iotas((8, HALF))
    norms = jnp.zeros((8, HALF), jnp.float32)
    for k in range(2):
        corner, both, diagonal = (
            (own_ref[rows, :] + other_ref[rows, :]) * (1.0 / 4096.0)
            for rows in (
                slice(k * 2 * HALF, k * 2 * HALF + HALF),
                slice(k * 2 * HALF + HALF, (k + 1) * 2 * HALF),
                slice(TAIL + k, TAIL + k + 1),
            )
        )
        stats = _unpack(corner, both, diagonal)
        parts = _split(stats)
        stats_ref[k] = stats
        square_ref[k] = _product(parts, parts)
        norms = jnp.where(norm_row == k, jnp.sum(stats * stats, axis=(0, 1), keepdims=True), norms)
        norms = jnp.where(norm_row == 2 + k, jnp.sum(jnp.where(row == col, stats, 0.0), axis=(0, 1), keepdims=True), norms)
    norms_ref[...] = norms


def _solve_kernel(where_ref, map_ref, stats_ref, square_ref, norms_ref, traces_ref, out_ref, first_ref):
    side = where_ref[0]
    pair = range(2)
    row, col = _iotas((ORDER, ORDER))
    on = row == col
    coupled, current, once = [], [], []
    for k in pair:
        held = map_ref[...] == where_ref[1 + k]
        members = jnp.sum(jnp.where(held, 0.5, 0.0), axis=(0, 1), keepdims=True)
        total = jnp.sum(jnp.where(held, traces_ref[...], 0.0), axis=(0, 1), keepdims=True) * (1.0 / 4096.0)
        ridge = 0.1 * total / (members * ORDER)
        squares = norms_ref[k : k + 1, 0:1] + ridge * (2.0 * norms_ref[2 + k : 3 + k, 0:1] + ORDER * ridge)
        scaled = 2.5 / jnp.sqrt(squares)
        coupled.append(scaled * (stats_ref[k] + jnp.where(on, ridge, 0.0)))
        first_ref[k] = jnp.sqrt(jnp.sqrt(scaled)) * (jnp.where(on, 1.25, 0.0) - 0.25 * coupled[k])
        square = (scaled * scaled) * (square_ref[k] + ((2.0 * ridge) * stats_ref[k] + jnp.where(on, ridge * ridge, 0.0)))
        once.append(0.0625 * square - 0.625 * coupled[k])
        current.append(jnp.concatenate([first_ref[k, pl.ds(q * 64 + side * 32, 32), :] for q in range(4)], 0))
    parts = [_split(coupled[k]) for k in pair]
    for step in range(ITERS - 1):
        if step > 0:
            once = [0.0625 * _product(parts[k], parts[k]) - 0.625 * coupled[k] for k in pair]
        split = [_split(once[k]) for k in pair]
        twice = [_split(3.125 * once[k] + _product(split[k], split[k])) for k in pair]
        coupled = [2.44140625 * coupled[k] + _product(twice[k], parts[k]) for k in pair]
        parts = [_split(coupled[k]) for k in pair]
        current = [1.25 * current[k] - 0.25 * _product(_split(current[k]), parts[k]) for k in pair]
    for k in pair:
        for c in range(2):
            for q in range(4):
                out_ref[c * 4 + q, k] = current[k][(q * 2 + c) * 16 : (q * 2 + c) * 16 + 16]


def _smem():
    return pl.BlockSpec(memory_space=pltpu.SMEM)


def _vmem():
    return pl.BlockSpec(memory_space=pltpu.VMEM)


def local(grads, layer_map):
    gradient = grads[0, :, 0]
    core, line, side = lax.axis_index("c"), lax.axis_index("y"), lax.axis_index("zh")
    holder = lax.axis_index(MP)
    half = gradient.shape[0] // 2
    pack = jax.ShapeDtypeStruct((half // 2, ROWS, HALF), jnp.float32)
    send, own = pl.pallas_call(
        _stats_kernel,
        out_shape=(pack, pack),
        in_specs=[_smem(), _vmem()],
        out_specs=(_vmem(), _vmem()),
        compiler_params=pltpu.CompilerParams(vmem_limit_bytes=16 * 2**20),
        name="stats",
    )(core.astype(jnp.int32).reshape(1), gradient)
    got = lax.ppermute(send, "c", [(0, 1), (1, 0)])
    chip = own + got
    pieces = lax.all_to_all(chip, "y", 0, 0, tiled=True)
    mine = jnp.sum(pieces, axis=0)
    other = lax.ppermute(mine, "zh", [(0, 1), (1, 0)])
    row = jnp.broadcast_to(mine[TAIL + 2][None, None], (64, 1, HALF))
    traces = lax.all_to_all(row, ("zh", "zl", "x"), 0, 0, tiled=True).reshape(64, HALF)
    layers = layer_map.reshape(2 * half, 32)
    layer_of = jnp.pad(jnp.tile(layers.T, (2, 1)), ((0, 0), (0, HALF - 2 * half)), constant_values=-1)
    block = core * half + line * 2
    pair = lax.dynamic_slice(layers, (block, holder), (2, 1)).reshape(2)
    whole = jax.ShapeDtypeStruct((half // 4, ORDER, ORDER), jnp.float32)
    prepared = pl.pallas_call(
        _prepare_kernel,
        out_shape=(whole, whole, jax.ShapeDtypeStruct((8, HALF), jnp.float32)),
        in_specs=[_vmem()] * 2,
        out_specs=(_vmem(),) * 3,
        compiler_params=pltpu.CompilerParams(vmem_limit_bytes=16 * 2**20),
        name="prepare",
    )(mine, other)
    rows = pl.pallas_call(
        _solve_kernel,
        out_shape=jax.ShapeDtypeStruct((8, half // 4, 16, ORDER), jnp.float32),
        in_specs=[_smem()] + [_vmem()] * 5,
        out_specs=_vmem(),
        scratch_shapes=[pltpu.VMEM((half // 4, ORDER, ORDER), jnp.float32)],
        compiler_params=pltpu.CompilerParams(vmem_limit_bytes=16 * 2**20),
        name="solve",
    )(jnp.concatenate([side.astype(jnp.int32).reshape(1), pair]), layer_of, *prepared, traces)
    back = lax.all_to_all(rows, ("c", "y"), 0, 0, tiled=True)
    return back.reshape(16, 1, 16, ORDER)


def solution(mesh):
    torus = Mesh(mesh.devices.reshape(4, 2, 2, 8, 4), ("y", "zh", "c", "zl", "x"))
    in_specs = (P(DP, None, MP, None, None), P())
    out_specs = P(None, MP, DP, None)
    return jax.shard_map(local, mesh=torus, in_specs=in_specs, out_specs=out_specs, check_vma=False)
```
